32 devices in a mesh: groups: 2 (over y), pages: 4 (over z), patches: 4 (over x, core).
Axes of the slice: x: 2, y: 2, z: 4, core: 2. Of those that a mesh axis runs over, the one named last changes fastest.
Arguments:
- queries: bfloat16 [16, 32, 128], P(('groups', 'pages'), 'patches'), parts along dimension 0, may hold values from -6 to 6
- gallery: bfloat16 [640, 1024, 128], P(('groups', 'pages'), 'patches'), parts along dimension 0, may hold values from -0.5 to 0.5
- page_rows: int32 [640], P('groups'), parts along dimension 0, may hold values from 0 to 319, as said below
- candidates: int32 [16, 32], P(('groups', 'pages')), parts along dimension 0, may hold values from 0 to 319, as said below
Outputs:
- scores: float32 [16, 32], P(('groups', 'pages')), parts along dimension 0
The draws below stay inside these ranges and needn't reach their ends.
There are 2 independent parts, one for each index of `groups`. The reference program is written for one: setup_inputs(seed, part) draws one part's arguments, and reference() takes and returns one part's arrays. A program takes and returns all parts, laid end to end along the dimension named above; each array names one. Nothing has to cross between parts.
Inputs may be any that keep to these rules, and one draw needn't show every extreme that they name: A permutation: page id c is stored at row page_rows[c] of gallery, which lies on pages index page_rows[c] // 80. Each query's 32 page ids are distinct. The 2 queries of one pages index have at most 48 candidates stored on one pages index, and in every draw some pages index stores exactly 48 candidates of the queries of every pages index.
All inputs are finite; a program needn't handle non-finite values.
Results may differ from the reference program's by a relative error of at most 0.0003.
Values may be sent and summed in bfloat16 or wider, within the bound.
A program may use at most 64 MiB of HBM per device.

```python
import jax
import jax.numpy as jnp
from jax import lax

DIM = 128
PATCH = 1024
QT = 32
CAND_OWN = 8
NQ_DEV = 2
PG_DEV = 80
CAND = 32
NQ = 8
PAGES = 320
N_PAGES = 4


def candidate_plan(key):
    owners = N_PAGES
    spots = 4 * CAND_OWN
    page_rows = jax.random.permutation(jax.random.fold_in(key, 101), PAGES).astype(jnp.int32)
    row_to_page = jnp.argsort(page_rows).astype(jnp.int32)
    hottest = jax.random.randint(jax.random.fold_in(key, 102), (), 0, owners)
    offsets = jax.random.randint(jax.random.fold_in(key, 103), (owners, NQ_DEV), 0, CAND_OWN)
    query_index = jnp.arange(NQ_DEV)
    signs = jnp.where(query_index % 2 == 0, 1, -1)
    signs = jnp.where((query_index % 2 == 0) & (query_index == NQ_DEV - 1), 0, signs)
    hot_counts = 3 * CAND_OWN + signs[None, :] * offsets[:, query_index // 2]
    limits = jax.random.randint(jax.random.fold_in(key, 104), (owners, NQ_DEV, owners), CAND_OWN, 3 * CAND_OWN + 1)
    is_hot = jnp.arange(owners) == hottest
    limits = jnp.where(is_hot[None, None, :], 0, limits)
    slot_index = jnp.arange(3 * CAND_OWN)
    open_slots = slot_index[None, None, None, :] < limits[..., None]
    noise = jax.random.randint(jax.random.fold_in(key, 105), open_slots.shape, 0, 2 ** 20)
    priority = jnp.where(open_slots, 2 ** 21, 0) + noise
    flat_priority = priority.reshape(owners, NQ_DEV, owners * 3 * CAND_OWN)
    ordering = jnp.argsort(-flat_priority, axis=-1)
    position = jnp.argsort(ordering, axis=-1)
    needed = CAND - hot_counts
    chosen = position < needed[..., None]
    counts = jnp.sum(chosen.reshape(owners, NQ_DEV, owners, 3 * CAND_OWN).astype(jnp.int32), axis=-1)
    counts = counts + jnp.where(is_hot[None, None, :], hot_counts[..., None], 0)
    local_noise = jax.random.randint(jax.random.fold_in(key, 106), (owners, NQ_DEV, owners, PG_DEV), 0, 2 ** 30)
    local_order = jnp.argsort(local_noise, axis=-1)[..., :spots].astype(jnp.int32)
    spot_index = jnp.arange(spots)
    usable = spot_index[None, None, None, :] < counts[..., None]
    storage = jnp.arange(owners, dtype=jnp.int32)[None, None, :, None] * PG_DEV + local_order
    flat_storage = storage.reshape(owners, NQ_DEV, owners * spots)
    flat_usable = usable.reshape(owners, NQ_DEV, owners * spots)
    shuffle = jax.random.randint(jax.random.fold_in(key, 107), flat_storage.shape, 0, 2 ** 20)
    sort_keys = jnp.where(flat_usable, 0, 2 ** 21) + shuffle
    taken = jnp.argsort(sort_keys, axis=-1)[..., :CAND]
    picked = jnp.take_along_axis(flat_storage, taken, axis=-1)
    candidates = row_to_page[picked].reshape(owners * NQ_DEV, CAND).astype(jnp.int32)
    return (page_rows, candidates)


def draw_page_rows(key, part):
    return candidate_plan(key)[0]


def draw_candidates(key, part):
    return candidate_plan(key)[1]


def level_of(rng, shape, shards, low, top_value):
    factor_of = 1.0
    for dim, parts in shards:
        heights = jax.random.uniform(jax.random.fold_in(jax.random.fold_in(rng, 6), dim), (parts,), jnp.float32, low / len(shards), top_value / len(shards))
        factor_of = factor_of * jnp.repeat(jnp.exp(heights), shape[dim] // parts).reshape((-1,) + (1,) * (len(shape) - 1 - dim))
    return factor_of


def centred(stream_key, extent, scale, reach, split=(), kind=jnp.bfloat16):
    drawn = jax.random.normal(stream_key, extent, jnp.float32) * scale
    if len(split) > 0:
        drawn = level_of(stream_key, extent, split, -0.22, 0.18) * drawn
    return jnp.clip(drawn, min=-reach, max=reach).astype(kind)


def setup_inputs(seed: int = 0, part: int = 0) -> dict:
    arg_keys = jax.random.split(jax.random.key(seed), 5)
    own_keys = jax.random.split(jax.random.fold_in(arg_keys[4], part), 5)
    queries = centred(own_keys[0], (NQ, QT, DIM), 1.0, 6.0, ((0, 4), (1, 4)))
    gallery = centred(own_keys[1], (PAGES, PATCH, DIM), DIM ** -0.5, 0.5, ((0, 4), (1, 4)))
    page_rows = draw_page_rows(jax.random.fold_in(jax.random.fold_in(arg_keys[4], part), 71), part)
    candidates = draw_candidates(jax.random.fold_in(jax.random.fold_in(arg_keys[4], part), 71), part)
    return dict(queries=queries, gallery=gallery, page_rows=page_rows, candidates=candidates)


def reference(queries, gallery, page_rows, candidates):
    rows = jnp.take(page_rows, candidates, axis=0).astype(jnp.int32)

    def per_query(item):
        tokens, row_ids = item
        pages = jnp.take(gallery, row_ids, axis=0).astype(jnp.float32)
        sims = jnp.einsum("td,cpd->ctp", tokens.astype(jnp.float32), pages, precision=lax.Precision.HIGHEST)
        return jnp.mean(jnp.max(sims, axis=2), axis=1)

    return lax.map(per_query, (queries, rows))
```

```python
import functools

import jax
import jax.numpy as jnp
from jax import lax
from jax.experimental import pallas as pl
from jax.experimental.pallas import tpu as pltpu
from jax.sharding import PartitionSpec as P

MESH = pl.DeviceIdType.MESH


def up(n, m):
    return -(-n // m) * m


def group_of(n, most):
    return max(d for d in range(1, most + 1) if n % d == 0)


def repeat(n, body):
    if n <= 16:
        for k in range(n):
            body(k)
    else:

        @pl.loop(0, n)
        def _(k):
            body(k)


def to_column(row):
    n = row.shape[1]
    eye = lax.broadcasted_iota(jnp.int32, (n, n), 0) == lax.broadcasted_iota(jnp.int32, (n, n), 1)
    return jnp.sum(jnp.where(eye, row, 0.0), axis=1, keepdims=True)


def to_row(column):
    n = column.shape[0]
    eye = lax.broadcasted_iota(jnp.int32, (n, n), 0) == lax.broadcasted_iota(jnp.int32, (n, n), 1)
    return jnp.sum(jnp.where(eye, column, 0.0), axis=0, keepdims=True)


def kernel(
    dims,
    q_ref,
    g_ref,
    rows_ref,
    cand_ref,
    out_ref,
    q_all,
    g_buf,
    best,
    best_in,
    send,
    arrived,
    g_sem,
    q_out,
    q_in,
    b_out,
    b_in,
    s_out,
    s_in,
):
    n_pages, n_patches, nq, tokens = dims
    devices = n_pages * n_patches
    page_count = g_ref.shape[0]
    share = page_count // n_patches
    me_g = lax.axis_index("groups")
    me_p = lax.axis_index("pages")
    me_j = lax.axis_index("patches")
    me = me_p * n_patches + me_j

    def owner(step):
        half = n_patches // 2
        chip, core = me_j // 2, lax.rem(me_j, 2)
        far = n_patches - 1 - step
        return lax.rem(chip + far // 2, half) * 2 + lax.rem(core + far, 2)

    def gallery_copy(step):
        first = owner(step) * share
        return pltpu.make_async_copy(
            g_ref.at[pl.ds(first, share)], g_buf.at[pl.ds(first, share)], g_sem.at[step]
        )

    for step in range(n_patches):
        gallery_copy(step).start()

    def peer(k):
        far = devices - 1 - k
        p = lax.rem(me_p + far // n_patches, n_pages)
        j = lax.rem(me_j + far % n_patches, n_patches)
        return p, j

    barrier = pltpu.get_barrier_semaphore()

    def greet(k):
        p, j = peer(k)
        pl.semaphore_signal(barrier, inc=1, device_id=(me_g, p, j), device_id_type=MESH)

    repeat(devices - 1, greet)

    q_all[me] = q_ref[...]
    send[...] = jnp.zeros_like(send)
    if best.shape[1] > share:
        best[:, share:, :] = jnp.zeros((best.shape[0], best.shape[1] - share, best.shape[2]), jnp.float32)
    page_rows = rows_ref[...].astype(jnp.float32)
    columns = []
    for q in range(nq):
        wanted = to_column(cand_ref[q : q + 1, :].astype(jnp.float32))
        ids = lax.broadcasted_iota(jnp.int32, (wanted.shape[0], page_rows.shape[1]), 1)
        hit = ids.astype(jnp.float32) == wanted
        columns.append(jnp.sum(jnp.where(hit, page_rows, 0.0), axis=1, keepdims=True))

    pl.semaphore_wait(barrier, devices - 1)

    def send_queries(k):
        p, j = peer(k)
        pltpu.make_async_remote_copy(
            src_ref=q_ref,
            dst_ref=q_all.at[me],
            send_sem=q_out,
            recv_sem=q_in,
            device_id=(me_g, p, j),
            device_id_type=MESH,
        ).start()

    repeat(devices - 1, send_queries)
    rest_q = q_all.at[pl.ds(0, devices - 1)]
    pltpu.make_async_copy(rest_q, rest_q, q_in).wait()

    unit = group_of(share, 5)
    token_rows = q_all[...].reshape(q_all.shape[0] * q_all.shape[1], q_all.shape[2])

    def best_copy(step):
        part = owner(step)
        return pltpu.make_async_remote_copy(
            src_ref=best.at[part],
            dst_ref=best_in.at[step],
            send_sem=b_out.at[step],
            recv_sem=b_in.at[step],
            device_id=(me_g, me_p, part),
            device_id_type=MESH,
        )

    for step in range(n_patches):
        part = owner(step)
        gallery_copy(step).wait()

        @pl.loop(0, share // unit)
        def _(block):
            for k in range(unit):
                page = block * unit + k
                sims = lax.dot_general(
                    g_buf[part * share + page],
                    token_rows,
                    (((1,), (1,)), ((), ())),
                    preferred_element_type=jnp.float32,
                )
                best[part, pl.ds(page, 1), :] = jnp.max(sims, axis=0, keepdims=True)

        if step < n_patches - 1:
            best_copy(step).start()

    width = best.shape[2]
    own_tokens = tokens // n_patches
    column = lax.broadcasted_iota(jnp.int32, (nq * n_pages, width), 1)
    query = lax.broadcasted_iota(jnp.int32, (nq * n_pages, width), 0)
    position = column // own_tokens
    named = position // (n_patches * nq) * nq + position % nq
    weights = jnp.where(named == query, 1.0 / tokens, 0.0)

    total = best[me_j]
    for step in range(n_patches - 1):
        best_copy(step).wait_recv()
        total = jnp.maximum(total, best_in[step])
    scores = lax.dot_general(
        weights,
        total,
        (((1,), (1,)), ((), ())),
        precision=lax.Precision.HIGHEST,
        preferred_element_type=jnp.float32,
    )
    for p in range(n_pages):
        send[p, :, : scores.shape[1]] = scores[p * nq : (p + 1) * nq, :]
    arrived[me] = send[me_p]

    def send_scores(k):
        p, j = peer(k)
        pltpu.make_async_remote_copy(
            src_ref=send.at[p],
            dst_ref=arrived.at[me],
            send_sem=s_out,
            recv_sem=s_in,
            device_id=(me_g, p, j),
            device_id_type=MESH,
        ).start()

    repeat(devices - 1, send_scores)
    rest_s = arrived.at[pl.ds(0, devices - 1)]
    pltpu.make_async_copy(rest_s, rest_s, s_in).wait()

    lanes = arrived.shape[2]
    spots = lax.broadcasted_iota(jnp.int32, (cand_ref.shape[1], lanes), 1).astype(jnp.float32)
    for q in range(nq):
        offset = columns[q] - spots

        def add(s, picked):
            first = jnp.float32(s * share) if isinstance(s, int) else (s * share).astype(jnp.float32)
            return picked + jnp.where(offset == first, arrived[s, q : q + 1, :], 0.0)

        picked = jnp.zeros(offset.shape, jnp.float32)
        if devices <= 16:
            for s in range(devices):
                picked = add(s, picked)
        else:
            picked = lax.fori_loop(0, devices, add, picked)
        out_ref[q : q + 1, :] = to_row(jnp.sum(picked, axis=1, keepdims=True))

    pltpu.make_async_copy(rest_q, rest_q, q_out).wait()
    for step in range(n_patches - 1):
        best_copy(step).wait_send()
    pltpu.make_async_copy(rest_s, rest_s, s_out).wait()


def body(queries, gallery, page_rows, candidates):
    nq, own_tokens, dim = queries.shape
    page_count, patches, _ = gallery.shape
    n_pages, n_patches = lax.axis_size("pages"), lax.axis_size("patches")
    devices = n_pages * n_patches
    share = page_count // n_patches
    rows = up(share, 8)
    width = devices * nq * own_tokens
    vmem = pl.BlockSpec(memory_space=pltpu.VMEM)
    dma = pltpu.SemaphoreType.DMA
    return pl.pallas_call(
        functools.partial(kernel, (n_pages, n_patches, nq, own_tokens * n_patches)),
        out_shape=jax.ShapeDtypeStruct(candidates.shape, jnp.float32),
        in_specs=[vmem, pl.BlockSpec(memory_space=pl.ANY), vmem, vmem],
        out_specs=vmem,
        scratch_shapes=[
            pltpu.VMEM((devices, nq * own_tokens, dim), jnp.bfloat16),
            pltpu.VMEM(gallery.shape, jnp.bfloat16),
            pltpu.VMEM((n_patches, rows, width), jnp.float32),
            pltpu.VMEM((n_patches, rows, width), jnp.float32),
            pltpu.VMEM((n_pages, nq, up(rows, 128)), jnp.float32),
            pltpu.VMEM((devices, nq, up(rows, 128)), jnp.float32),
            dma((n_patches,)),
            dma,
            dma,
            dma((n_patches,)),
            dma((n_patches,)),
            dma,
            dma,
        ],
        compiler_params=pltpu.CompilerParams(collective_id=0, has_side_effects=True),
    )(
        queries.reshape(nq * own_tokens, dim),
        gallery,
        page_rows.reshape(1, -1),
        candidates,
    )


def solution(mesh):
    in_specs = (
        P(("groups", "pages"), "patches", None),
        P(("groups", "pages"), "patches", None),
        P("groups"),
        P(("groups", "pages"), None),
    )
    out_specs = P(("groups", "pages"), None)
    return jax.shard_map(body, mesh=mesh, in_specs=in_specs, out_specs=out_specs, check_vma=False)
```

```python
import functools

import jax
import jax.numpy as jnp
from jax import lax
from jax.experimental import pallas as pl
from jax.experimental.pallas import tpu as pltpu
from jax.sharding import PartitionSpec as P

MESH = pl.DeviceIdType.MESH


def up(n, m):
    return -(-n // m) * m


def group_of(n, most):
    return max(d for d in range(1, most + 1) if n % d == 0)


def repeat(n, body):
    if n <= 16:
        for k in range(n):
            body(k)
    else:

        @pl.loop(0, n)
        def _(k):
            body(k)


def to_column(row):
    n = row.shape[1]
    eye = lax.broadcasted_iota(jnp.int32, (n, n), 0) == lax.broadcasted_iota(jnp.int32, (n, n), 1)
    return jnp.sum(jnp.where(eye, row, 0.0), axis=1, keepdims=True)


def to_row(column):
    n = column.shape[0]
    eye = lax.broadcasted_iota(jnp.int32, (n, n), 0) == lax.broadcasted_iota(jnp.int32, (n, n), 1)
    return jnp.sum(jnp.where(eye, column, 0.0), axis=0, keepdims=True)


def kernel(
    dims,
    q_hbm,
    g_ref,
    rows_hbm,
    cand_hbm,
    out_ref,
    q_ref,
    rows_ref,
    cand_ref,
    q_all,
    g_buf,
    best,
    best_in,
    send,
    arrived,
    g_sem,
    a_sem,
    q_out,
    q_in,
    b_out,
    b_in,
    s_out,
    s_in,
):
    n_pages, n_patches, nq, tokens = dims
    devices = n_pages * n_patches
    page_count = g_ref.shape[0]
    share = page_count // n_patches
    me_g = lax.axis_index("groups")
    me_p = lax.axis_index("pages")
    me_j = lax.axis_index("patches")
    me = me_p * n_patches + me_j

    def owner(step):
        half = n_patches // 2
        chip, core = me_j // 2, lax.rem(me_j, 2)
        far = n_patches - 1 - step
        return lax.rem(chip + far // 2, half) * 2 + lax.rem(core + far, 2)

    def gallery_copy(step):
        first = owner(step) * share
        return pltpu.make_async_copy(
            g_ref.at[pl.ds(first, share)], g_buf.at[pl.ds(first, share)], g_sem.at[step]
        )

    def peer(k):
        far = devices - 1 - k
        p = lax.rem(me_p + far // n_patches, n_pages)
        j = lax.rem(me_j + far % n_patches, n_patches)
        return p, j

    barrier = pltpu.get_barrier_semaphore()

    def greet(k):
        p, j = peer(k)
        pl.semaphore_signal(barrier, inc=1, device_id=(me_g, p, j), device_id_type=MESH)

    repeat(devices - 1, greet)
    small = [
        pltpu.make_async_copy(source, target, a_sem.at[k])
        for k, (source, target) in enumerate(
            ((q_hbm, q_ref), (cand_hbm, cand_ref), (rows_hbm, rows_ref))
        )
    ]
    for copy in small:
        copy.start()
    for step in range(n_patches):
        gallery_copy(step).start()
    send[...] = jnp.zeros_like(send)
    if best.shape[1] > share:
        best[:, share:, :] = jnp.zeros((best.shape[0], best.shape[1] - share, best.shape[2]), jnp.float32)
    for copy in small:
        copy.wait()

    q_all[me] = q_ref[...]
    page_rows = rows_ref[...].astype(jnp.float32).reshape(1, -1)
    columns = []
    for q in range(nq):
        wanted = to_column(cand_ref[q : q + 1, :].astype(jnp.float32))
        ids = lax.broadcasted_iota(jnp.int32, (wanted.shape[0], page_rows.shape[1]), 1)
        hit = ids.astype(jnp.float32) == wanted
        columns.append(jnp.sum(jnp.where(hit, page_rows, 0.0), axis=1, keepdims=True))

    pl.semaphore_wait(barrier, devices - 1)

    def send_queries(k):
        p, j = peer(k)
        pltpu.make_async_remote_copy(
            src_ref=q_ref,
            dst_ref=q_all.at[me],
            send_sem=q_out,
            recv_sem=q_in,
            device_id=(me_g, p, j),
            device_id_type=MESH,
        ).start()

    repeat(devices - 1, send_queries)
    rest_q = q_all.at[pl.ds(0, devices - 1)]
    pltpu.make_async_copy(rest_q, rest_q, q_in).wait()

    unit = group_of(share, 20)
    token_rows = q_all[...].reshape(q_all.shape[0] * q_all.shape[1], q_all.shape[2])

    def best_copy(step):
        part = owner(step)
        return pltpu.make_async_remote_copy(
            src_ref=best.at[part],
            dst_ref=best_in.at[step],
            send_sem=b_out.at[step],
            recv_sem=b_in.at[step],
            device_id=(me_g, me_p, part),
            device_id_type=MESH,
        )

    for step in range(n_patches):
        part = owner(step)
        gallery_copy(step).wait()

        def block(start):
            for k in range(unit):
                page = start + k
                sims = lax.dot_general(
                    g_buf[part * share + page],
                    token_rows,
                    (((1,), (1,)), ((), ())),
                    preferred_element_type=jnp.float32,
                )
                best[part, pl.ds(page, 1), :] = jnp.max(sims, axis=0, keepdims=True)

        if unit == share:
            block(0)
        else:
            pl.loop(0, share, step=unit)(block)

        if step < n_patches - 1:
            best_copy(step).start()

    width = best.shape[2]
    own_tokens = tokens // n_patches
    column = lax.broadcasted_iota(jnp.int32, (nq * n_pages, width), 1)
    query = lax.broadcasted_iota(jnp.int32, (nq * n_pages, width), 0)
    position = column // own_tokens
    named = position // (n_patches * nq) * nq + position % nq
    weights = jnp.where(named == query, 1.0 / tokens, 0.0)

    total = best[me_j]
    for step in range(n_patches - 1):
        best_copy(step).wait_recv()
        total = jnp.maximum(total, best_in[step])
    scores = lax.dot_general(
        weights,
        total,
        (((1,), (1,)), ((), ())),
        precision=lax.Precision.HIGHEST,
        preferred_element_type=jnp.float32,
    )
    for p in range(n_pages):
        send[p, :, : scores.shape[1]] = scores[p * nq : (p + 1) * nq, :]
    arrived[me] = send[me_p]

    def send_scores(k):
        p, j = peer(k)
        pltpu.make_async_remote_copy(
            src_ref=send.at[p],
            dst_ref=arrived.at[me],
            send_sem=s_out,
            recv_sem=s_in,
            device_id=(me_g, p, j),
            device_id_type=MESH,
        ).start()

    repeat(devices - 1, send_scores)
    rest_s = arrived.at[pl.ds(0, devices - 1)]
    pltpu.make_async_copy(rest_s, rest_s, s_in).wait()

    lanes = arrived.shape[2]
    spots = lax.broadcasted_iota(jnp.int32, (cand_ref.shape[1], lanes), 1).astype(jnp.float32)
    for q in range(nq):
        offset = columns[q] - spots

        def add(s, picked):
            first = jnp.float32(s * share) if isinstance(s, int) else (s * share).astype(jnp.float32)
            return picked + jnp.where(offset == first, arrived[s, q : q + 1, :], 0.0)

        picked = jnp.zeros(offset.shape, jnp.float32)
        if devices <= 16:
            for s in range(devices):
                picked = add(s, picked)
        else:
            picked = lax.fori_loop(0, devices, add, picked)
        out_ref[q : q + 1, :] = to_row(jnp.sum(picked, axis=1, keepdims=True))

    pltpu.make_async_copy(rest_q, rest_q, q_out).wait()
    for step in range(n_patches - 1):
        best_copy(step).wait_send()
    pltpu.make_async_copy(rest_s, rest_s, s_out).wait()


def body(queries, gallery, page_rows, candidates):
    nq, own_tokens, dim = queries.shape
    page_count, patches, _ = gallery.shape
    n_pages, n_patches = lax.axis_size("pages"), lax.axis_size("patches")
    devices = n_pages * n_patches
    share = page_count // n_patches
    rows = up(share, 8)
    width = devices * nq * own_tokens
    vmem = pl.BlockSpec(memory_space=pltpu.VMEM)
    dma = pltpu.SemaphoreType.DMA
    return pl.pallas_call(
        functools.partial(kernel, (n_pages, n_patches, nq, own_tokens * n_patches)),
        out_shape=pltpu.VMEM(candidates.shape, jnp.float32),
        in_specs=[pl.BlockSpec(memory_space=pl.ANY)] * 4,
        out_specs=vmem,
        scratch_shapes=[
            pltpu.VMEM((nq * own_tokens, dim), jnp.bfloat16),
            pltpu.VMEM(page_rows.shape, jnp.int32),
            pltpu.VMEM(candidates.shape, jnp.int32),
            pltpu.VMEM((devices, nq * own_tokens, dim), jnp.bfloat16),
            pltpu.VMEM(gallery.shape, jnp.bfloat16),
            pltpu.VMEM((n_patches, rows, width), jnp.float32),
            pltpu.VMEM((n_patches, rows, width), jnp.float32),
            pltpu.VMEM((n_pages, nq, up(rows, 128)), jnp.float32),
            pltpu.VMEM((devices, nq, up(rows, 128)), jnp.float32),
            dma((n_patches,)),
            dma((3,)),
            dma,
            dma,
            dma((n_patches,)),
            dma((n_patches,)),
            dma,
            dma,
        ],
        compiler_params=pltpu.CompilerParams(collective_id=0, has_side_effects=True),
    )(
        queries.reshape(nq * own_tokens, dim),
        gallery,
        page_rows,
        candidates,
    )


def solution(mesh):
    in_specs = (
        P(("groups", "pages"), "patches", None),
        P(("groups", "pages"), "patches", None),
        P("groups"),
        P(("groups", "pages"), None),
    )
    out_specs = P(("groups", "pages"), None)
    return jax.shard_map(body, mesh=mesh, in_specs=in_specs, out_specs=out_specs, check_vma=False)
```

```python
import functools

import jax
import jax.numpy as jnp
from jax import lax
from jax.experimental import pallas as pl
from jax.experimental.pallas import tpu as pltpu
from jax.sharding import PartitionSpec as P

MESH = pl.DeviceIdType.MESH


def up(n, m):
    return -(-n // m) * m


def group_of(n, most):
    return max(d for d in range(1, most + 1) if n % d == 0)


def repeat(n, body):
    if n <= 16:
        for k in range(n):
            body(k)
    else:

        @pl.loop(0, n)
        def _(k):
            body(k)


def to_column(row):
    n = row.shape[1]
    eye = lax.broadcasted_iota(jnp.int32, (n, n), 0) == lax.broadcasted_iota(jnp.int32, (n, n), 1)
    return jnp.sum(jnp.where(eye, row, 0.0), axis=1, keepdims=True)


def to_row(column):
    n = column.shape[0]
    eye = lax.broadcasted_iota(jnp.int32, (n, n), 0) == lax.broadcasted_iota(jnp.int32, (n, n), 1)
    return jnp.sum(jnp.where(eye, column, 0.0), axis=0, keepdims=True)


def top_row(sims):
    rows, width = sims.shape
    chains = 4
    if rows % (8 * chains) == 0:
        sims = jnp.max(sims.reshape(rows // (8 * chains), chains, 8, width), axis=0)
        sims = jnp.maximum(jnp.maximum(sims[0], sims[1]), jnp.maximum(sims[2], sims[3]))
    return jnp.max(sims, axis=0, keepdims=True)


def kernel(
    dims,
    q_hbm,
    g_ref,
    rows_hbm,
    cand_hbm,
    out_ref,
    q_ref,
    rows_ref,
    cand_ref,
    q_all,
    g_buf,
    best,
    best_in,
    send,
    arrived,
    g_sem,
    a_sem,
    q_out,
    q_in,
    b_out,
    b_in,
    s_out,
    s_in,
):
    n_pages, n_patches, nq, tokens = dims
    devices = n_pages * n_patches
    page_count = g_ref.shape[0]
    share = page_count // n_patches
    me_g = lax.axis_index("groups")
    me_p = lax.axis_index("pages")
    me_j = lax.axis_index("patches")
    me = me_p * n_patches + me_j

    def owner(step):
        half = n_patches // 2
        chip, core = me_j // 2, lax.rem(me_j, 2)
        far = n_patches - 1 - step
        return lax.rem(chip + far // 2, half) * 2 + lax.rem(core + far, 2)

    def gallery_copy(step):
        first = owner(step) * share
        return pltpu.make_async_copy(
            g_ref.at[pl.ds(first, share)], g_buf.at[pl.ds(first, share)], g_sem.at[step]
        )

    def peer(k):
        far = devices - 1 - k
        p = lax.rem(me_p + far // n_patches, n_pages)
        j = lax.rem(me_j + far % n_patches, n_patches)
        return p, j

    barrier = pltpu.get_barrier_semaphore()

    def greet(k):
        p, j = peer(k)
        pl.semaphore_signal(barrier, inc=1, device_id=(me_g, p, j), device_id_type=MESH)

    repeat(devices - 1, greet)
    small = [
        pltpu.make_async_copy(source, target, a_sem.at[k])
        for k, (source, target) in enumerate(
            ((q_hbm, q_ref), (cand_hbm, cand_ref), (rows_hbm, rows_ref))
        )
    ]
    for copy in small:
        copy.start()
    for step in range(n_patches):
        gallery_copy(step).start()
    send[...] = jnp.zeros_like(send)
    if best.shape[2] > share:
        spare = best.at[:, :, share:, :]
        spare[...] = jnp.zeros(spare.shape, jnp.float32)
    for copy in small:
        copy.wait()

    q_all[me] = q_ref[...]
    page_rows = rows_ref[...].astype(jnp.float32).reshape(1, -1)
    columns = []
    for q in range(nq):
        wanted = to_column(cand_ref[q : q + 1, :].astype(jnp.float32))
        ids = lax.broadcasted_iota(jnp.int32, (wanted.shape[0], page_rows.shape[1]), 1)
        hit = ids.astype(jnp.float32) == wanted
        columns.append(jnp.sum(jnp.where(hit, page_rows, 0.0), axis=1, keepdims=True))

    pl.semaphore_wait(barrier, devices - 1)

    half_pages = n_pages // 2
    half_devices = devices // 2
    my_half = me_p // half_pages

    def send_queries(k):
        p, j = peer(k)
        pltpu.make_async_remote_copy(
            src_ref=q_ref,
            dst_ref=q_all.at[me],
            send_sem=q_out,
            recv_sem=q_in.at[lax.rem(p // half_pages + my_half, 2)],
            device_id=(me_g, p, j),
            device_id_type=MESH,
        ).start()

    repeat(devices - 1, send_queries)
    rest_q = q_all.at[pl.ds(0, devices - 1)]

    unit = group_of(share, 20)

    def half_weights(half, others):
        some = q_all.at[pl.ds(0, others)]
        pltpu.make_async_copy(some, some, q_in.at[0 if others < half_devices else 1]).wait()
        rows = q_all[pl.ds(half * half_devices, half_devices)]
        rows = rows.reshape(rows.shape[0] * rows.shape[1], rows.shape[2])
        none = jnp.zeros_like(rows)
        return jnp.concatenate(
            [jnp.concatenate([rows, none], axis=1), jnp.concatenate([none, rows], axis=1)], axis=0
        )

    def part_maxima(part, half, weights):
        def block(start):
            for k in range(0, unit, 2):
                first, second = start + k, start + min(k + 1, unit - 1)
                pair = jnp.concatenate(
                    [g_buf[part * share + first], g_buf[part * share + second]], axis=1
                )
                sims = lax.dot_general(
                    pair, weights, (((1,), (1,)), ((), ())), preferred_element_type=jnp.float32
                )
                row = top_row(sims)
                width = row.shape[1] // 2
                best[part, half, pl.ds(first, 1), :] = row[:, :width]
                best[part, half, pl.ds(second, 1), :] = row[:, width:]

        if unit == share:
            block(0)
        else:
            pl.loop(0, share, step=unit)(block)

    def best_copy(step):
        part = owner(step)
        return pltpu.make_async_remote_copy(
            src_ref=best.at[part],
            dst_ref=best_in.at[step],
            send_sem=b_out.at[step],
            recv_sem=b_in.at[step],
            device_id=(me_g, me_p, part),
            device_id_type=MESH,
        )

    weights = half_weights(my_half, half_devices - 1)
    for step in range(n_patches):
        gallery_copy(step).wait()
        part_maxima(owner(step), my_half, weights)
    weights = half_weights(1 - my_half, half_devices)
    for step in range(n_patches):
        part_maxima(owner(step), 1 - my_half, weights)
        if step < n_patches - 1:
            best_copy(step).start()

    width = 2 * best.shape[3]
    own_tokens = tokens // n_patches
    column = lax.broadcasted_iota(jnp.int32, (nq * n_pages, width), 1)
    query = lax.broadcasted_iota(jnp.int32, (nq * n_pages, width), 0)
    position = column // own_tokens
    named = position // (n_patches * nq) * nq + position % nq
    weights = jnp.where(named == query, 1.0 / tokens, 0.0)

    total = best[me_j]
    for step in range(n_patches - 1):
        best_copy(step).wait_recv()
        total = jnp.maximum(total, best_in[step])
    scores = sum(
        lax.dot_general(
            weights[:, half * best.shape[3] : (half + 1) * best.shape[3]],
            total[half],
            (((1,), (1,)), ((), ())),
            precision=lax.Precision.HIGHEST,
            preferred_element_type=jnp.float32,
        )
        for half in range(2)
    )
    for p in range(n_pages):
        send[p, :, : scores.shape[1]] = scores[p * nq : (p + 1) * nq, :]
    arrived[me] = send[me_p]

    def send_scores(k):
        p, j = peer(k)
        pltpu.make_async_remote_copy(
            src_ref=send.at[p],
            dst_ref=arrived.at[me],
            send_sem=s_out,
            recv_sem=s_in,
            device_id=(me_g, p, j),
            device_id_type=MESH,
        ).start()

    repeat(devices - 1, send_scores)
    rest_s = arrived.at[pl.ds(0, devices - 1)]
    pltpu.make_async_copy(rest_s, rest_s, s_in).wait()

    lanes = arrived.shape[2]
    spots = lax.broadcasted_iota(jnp.int32, (cand_ref.shape[1], lanes), 1).astype(jnp.float32)
    for q in range(nq):
        offset = columns[q] - spots

        def add(s, picked):
            first = jnp.float32(s * share) if isinstance(s, int) else (s * share).astype(jnp.float32)
            return picked + jnp.where(offset == first, arrived[s, q : q + 1, :], 0.0)

        picked = jnp.zeros(offset.shape, jnp.float32)
        if devices <= 16:
            for s in range(devices):
                picked = add(s, picked)
        else:
            picked = lax.fori_loop(0, devices, add, picked)
        out_ref[q : q + 1, :] = to_row(jnp.sum(picked, axis=1, keepdims=True))

    pltpu.make_async_copy(rest_q, rest_q, q_out).wait()
    for step in range(n_patches - 1):
        best_copy(step).wait_send()
    pltpu.make_async_copy(rest_s, rest_s, s_out).wait()


def body(queries, gallery, page_rows, candidates):
    nq, own_tokens, dim = queries.shape
    page_count, patches, _ = gallery.shape
    n_pages, n_patches = lax.axis_size("pages"), lax.axis_size("patches")
    devices = n_pages * n_patches
    share = page_count // n_patches
    rows = up(share, 8)
    width = devices * nq * own_tokens
    vmem = pl.BlockSpec(memory_space=pltpu.VMEM)
    dma = pltpu.SemaphoreType.DMA
    return pl.pallas_call(
        functools.partial(kernel, (n_pages, n_patches, nq, own_tokens * n_patches)),
        out_shape=pltpu.VMEM(candidates.shape, jnp.float32),
        in_specs=[pl.BlockSpec(memory_space=pl.ANY)] * 4,
        out_specs=vmem,
        scratch_shapes=[
            pltpu.VMEM((nq * own_tokens, dim), jnp.bfloat16),
            pltpu.VMEM(page_rows.shape, jnp.int32),
            pltpu.VMEM(candidates.shape, jnp.int32),
            pltpu.VMEM((devices, nq * own_tokens, dim), jnp.bfloat16),
            pltpu.VMEM(gallery.shape, jnp.bfloat16),
            pltpu.VMEM((n_patches, 2, rows, width // 2), jnp.float32),
            pltpu.VMEM((n_patches, 2, rows, width // 2), jnp.float32),
            pltpu.VMEM((n_pages, nq, up(rows, 128)), jnp.float32),
            pltpu.VMEM((devices, nq, up(rows, 128)), jnp.float32),
            dma((n_patches,)),
            dma((3,)),
            dma,
            dma((2,)),
            dma((n_patches,)),
            dma((n_patches,)),
            dma,
            dma,
        ],
        compiler_params=pltpu.CompilerParams(collective_id=0, has_side_effects=True),
    )(
        queries.reshape(nq * own_tokens, dim),
        gallery,
        page_rows,
        candidates,
    )


def solution(mesh):
    in_specs = (
        P(("groups", "pages"), "patches", None),
        P(("groups", "pages"), "patches", None),
        P("groups"),
        P(("groups", "pages"), None),
    )
    out_specs = P(("groups", "pages"), None)
    return jax.shard_map(body, mesh=mesh, in_specs=in_specs, out_specs=out_specs, check_vma=False)
```

```python
import functools

import jax
import jax.numpy as jnp
from jax import lax
from jax.experimental import pallas as pl
from jax.experimental.pallas import tpu as pltpu
from jax.sharding import PartitionSpec as P

MESH = pl.DeviceIdType.MESH


def up(n, m):
    return -(-n // m) * m


def group_of(n, most):
    return max(d for d in range(1, most + 1) if n % d == 0)


def repeat(n, body):
    if n <= 16:
        for k in range(n):
            body(k)
    else:

        @pl.loop(0, n)
        def _(k):
            body(k)


def to_column(row):
    n = row.shape[1]
    eye = lax.broadcasted_iota(jnp.int32, (n, n), 0) == lax.broadcasted_iota(jnp.int32, (n, n), 1)
    return jnp.sum(jnp.where(eye, row, 0.0), axis=1, keepdims=True)


def to_row(column):
    n = column.shape[0]
    eye = lax.broadcasted_iota(jnp.int32, (n, n), 0) == lax.broadcasted_iota(jnp.int32, (n, n), 1)
    return jnp.sum(jnp.where(eye, column, 0.0), axis=0, keepdims=True)


def top_row(sims):
    rows, width = sims.shape
    chains = 4
    if rows % (8 * chains) == 0:
        sims = jnp.max(sims.reshape(rows // (8 * chains), chains, 8, width), axis=0)
        sims = jnp.maximum(jnp.maximum(sims[0], sims[1]), jnp.maximum(sims[2], sims[3]))
    return jnp.max(sims, axis=0, keepdims=True)


def kernel(
    dims,
    q_hbm,
    g_ref,
    rows_hbm,
    cand_hbm,
    out_ref,
    q_ref,
    rows_ref,
    cand_ref,
    q_all,
    g_buf,
    best,
    best_in,
    send,
    arrived,
    g_sem,
    a_sem,
    q_out,
    q_in,
    b_out,
    b_in,
    s_out,
    s_in,
):
    n_pages, n_patches, nq, tokens = dims
    devices = n_pages * n_patches
    page_count = g_ref.shape[0]
    share = page_count // n_patches
    me_g = lax.axis_index("groups")
    me_p = lax.axis_index("pages")
    me_j = lax.axis_index("patches")
    me = me_p * n_patches + me_j

    def owner(step):
        half = n_patches // 2
        chip, core = me_j // 2, lax.rem(me_j, 2)
        far = n_patches - 1 - step
        return lax.rem(chip + far // 2, half) * 2 + lax.rem(core + far, 2)

    def gallery_copy(step):
        first = owner(step) * share
        return pltpu.make_async_copy(
            g_ref.at[pl.ds(first, share)], g_buf.at[pl.ds(first, share)], g_sem.at[step]
        )

    def peer(k):
        far = devices - 1 - k
        p = lax.rem(me_p + far // n_patches, n_pages)
        j = lax.rem(me_j + far % n_patches, n_patches)
        return p, j

    barrier = pltpu.get_barrier_semaphore()

    def greet(k):
        p, j = peer(k)
        pl.semaphore_signal(barrier, inc=1, device_id=(me_g, p, j), device_id_type=MESH)

    repeat(devices - 1, greet)
    small = [
        pltpu.make_async_copy(source, target, a_sem.at[k])
        for k, (source, target) in enumerate(
            ((q_hbm, q_ref), (cand_hbm, cand_ref), (rows_hbm, rows_ref))
        )
    ]
    for copy in small:
        copy.start()
    for step in range(n_patches):
        gallery_copy(step).start()
    send[...] = jnp.zeros_like(send)
    if best.shape[2] > share:
        spare = best.at[:, :, share:, :]
        spare[...] = jnp.zeros(spare.shape, jnp.float32)
    for copy in small:
        copy.wait()

    q_all[me] = q_ref[...]
    page_rows = rows_ref[...].astype(jnp.float32).reshape(1, -1)
    columns = []
    for q in range(nq):
        wanted = to_column(cand_ref[q : q + 1, :].astype(jnp.float32))
        ids = lax.broadcasted_iota(jnp.int32, (wanted.shape[0], page_rows.shape[1]), 1)
        hit = ids.astype(jnp.float32) == wanted
        columns.append(jnp.sum(jnp.where(hit, page_rows, 0.0), axis=1, keepdims=True))

    pl.semaphore_wait(barrier, devices - 1)

    half_pages = n_pages // 2
    half_devices = devices // 2
    my_half = me_p // half_pages

    def send_queries(k):
        p, j = peer(k)
        pltpu.make_async_remote_copy(
            src_ref=q_ref,
            dst_ref=q_all.at[me],
            send_sem=q_out,
            recv_sem=q_in.at[lax.rem(p // half_pages + my_half, 2)],
            device_id=(me_g, p, j),
            device_id_type=MESH,
        ).start()

    repeat(devices - 1, send_queries)
    rest_q = q_all.at[pl.ds(0, devices - 1)]

    unit = group_of(share, 20)

    def half_weights(half, others):
        some = q_all.at[pl.ds(0, others)]
        pltpu.make_async_copy(some, some, q_in.at[0 if others < half_devices else 1]).wait()
        rows = q_all[pl.ds(half * half_devices, half_devices)]
        rows = rows.reshape(rows.shape[0] * rows.shape[1], rows.shape[2])
        none = jnp.zeros_like(rows)
        return jnp.concatenate(
            [jnp.concatenate([rows, none], axis=1), jnp.concatenate([none, rows], axis=1)], axis=0
        )

    def part_maxima(part, half, weights):
        def block(start):
            for k in range(0, unit, 2):
                first, second = start + k, start + min(k + 1, unit - 1)
                pair = jnp.concatenate(
                    [g_buf[part * share + first], g_buf[part * share + second]], axis=1
                )
                sims = lax.dot_general(
                    pair, weights, (((1,), (1,)), ((), ())), preferred_element_type=jnp.float32
                )
                row = top_row(sims)
                width = row.shape[1] // 2
                best[part, half, pl.ds(first, 1), :] = row[:, :width]
                best[part, half, pl.ds(second, 1), :] = row[:, width:]

        if unit == share:
            block(0)
        else:
            pl.loop(0, share, step=unit)(block)

    def best_copy(step):
        part = owner(step)
        return pltpu.make_async_remote_copy(
            src_ref=best.at[part],
            dst_ref=best_in.at[step],
            send_sem=b_out.at[step],
            recv_sem=b_in.at[step],
            device_id=(me_g, me_p, part),
            device_id_type=MESH,
        )

    for step in range(n_patches):
        gallery_copy(step).wait()
    weights = half_weights(my_half, half_devices - 1)
    for step in range(n_patches):
        part_maxima(owner(step), my_half, weights)
    weights = half_weights(1 - my_half, half_devices)
    for step in range(n_patches):
        part_maxima(owner(step), 1 - my_half, weights)
        if step < n_patches - 1:
            best_copy(step).start()

    width = 2 * best.shape[3]
    own_tokens = tokens // n_patches
    column = lax.broadcasted_iota(jnp.int32, (nq * n_pages, width), 1)
    query = lax.broadcasted_iota(jnp.int32, (nq * n_pages, width), 0)
    position = column // own_tokens
    named = position // (n_patches * nq) * nq + position % nq
    weights = jnp.where(named == query, 1.0 / tokens, 0.0)

    total = best[me_j]
    for step in range(n_patches - 1):
        best_copy(step).wait_recv()
        total = jnp.maximum(total, best_in[step])
    scores = sum(
        lax.dot_general(
            weights[:, half * best.shape[3] : (half + 1) * best.shape[3]],
            total[half],
            (((1,), (1,)), ((), ())),
            precision=lax.Precision.HIGHEST,
            preferred_element_type=jnp.float32,
        )
        for half in range(2)
    )
    for p in range(n_pages):
        send[p, :, : scores.shape[1]] = scores[p * nq : (p + 1) * nq, :]
    arrived[me] = send[me_p]

    def send_scores(k):
        p, j = peer(k)
        pltpu.make_async_remote_copy(
            src_ref=send.at[p],
            dst_ref=arrived.at[me],
            send_sem=s_out,
            recv_sem=s_in,
            device_id=(me_g, p, j),
            device_id_type=MESH,
        ).start()

    repeat(devices - 1, send_scores)
    rest_s = arrived.at[pl.ds(0, devices - 1)]
    pltpu.make_async_copy(rest_s, rest_s, s_in).wait()

    lanes = arrived.shape[2]
    spots = lax.broadcasted_iota(jnp.int32, (cand_ref.shape[1], lanes), 1).astype(jnp.float32)
    for q in range(nq):
        offset = columns[q] - spots

        def add(s, picked):
            first = jnp.float32(s * share) if isinstance(s, int) else (s * share).astype(jnp.float32)
            return picked + jnp.where(offset == first, arrived[s, q : q + 1, :], 0.0)

        picked = jnp.zeros(offset.shape, jnp.float32)
        if devices <= 16:
            for s in range(devices):
                picked = add(s, picked)
        else:
            picked = lax.fori_loop(0, devices, add, picked)
        out_ref[q : q + 1, :] = to_row(jnp.sum(picked, axis=1, keepdims=True))

    pltpu.make_async_copy(rest_q, rest_q, q_out).wait()
    for step in range(n_patches - 1):
        best_copy(step).wait_send()
    pltpu.make_async_copy(rest_s, rest_s, s_out).wait()


def body(queries, gallery, page_rows, candidates):
    nq, own_tokens, dim = queries.shape
    page_count, patches, _ = gallery.shape
    n_pages, n_patches = lax.axis_size("pages"), lax.axis_size("patches")
    devices = n_pages * n_patches
    share = page_count // n_patches
    rows = up(share, 8)
    width = devices * nq * own_tokens
    vmem = pl.BlockSpec(memory_space=pltpu.VMEM)
    dma = pltpu.SemaphoreType.DMA
    return pl.pallas_call(
        functools.partial(kernel, (n_pages, n_patches, nq, own_tokens * n_patches)),
        out_shape=pltpu.VMEM(candidates.shape, jnp.float32),
        in_specs=[pl.BlockSpec(memory_space=pl.ANY)] * 4,
        out_specs=vmem,
        scratch_shapes=[
            pltpu.VMEM((nq * own_tokens, dim), jnp.bfloat16),
            pltpu.VMEM(page_rows.shape, jnp.int32),
            pltpu.VMEM(candidates.shape, jnp.int32),
            pltpu.VMEM((devices, nq * own_tokens, dim), jnp.bfloat16),
            pltpu.VMEM(gallery.shape, jnp.bfloat16),
            pltpu.VMEM((n_patches, 2, rows, width // 2), jnp.float32),
            pltpu.VMEM((n_patches, 2, rows, width // 2), jnp.float32),
            pltpu.VMEM((n_pages, nq, up(rows, 128)), jnp.float32),
            pltpu.VMEM((devices, nq, up(rows, 128)), jnp.float32),
            dma((n_patches,)),
            dma((3,)),
            dma,
            dma((2,)),
            dma((n_patches,)),
            dma((n_patches,)),
            dma,
            dma,
        ],
        compiler_params=pltpu.CompilerParams(collective_id=0, has_side_effects=True),
    )(
        queries.reshape(nq * own_tokens, dim),
        gallery,
        page_rows,
        candidates,
    )


def solution(mesh):
    in_specs = (
        P(("groups", "pages"), "patches", None),
        P(("groups", "pages"), "patches", None),
        P("groups"),
        P(("groups", "pages"), None),
    )
    out_specs = P(("groups", "pages"), None)
    return jax.shard_map(body, mesh=mesh, in_specs=in_specs, out_specs=out_specs, check_vma=False)
```
